32 devices in a mesh: cuts: 2 (over x), ma: 8 (over z, y), mb: 2 (over core).
Axes of the slice: x: 2, y: 2, z: 4, core: 2. Of those that a mesh axis runs over, the one named last changes fastest.
Arguments:
- stem_field: bfloat16 [64, 512, 2, 512], P(('cuts', 'ma', 'mb')), parts along dimension 0, may hold values from -6 to 6
- first_branch_tensors: bfloat16 [2, 2, 512, 512], P(None, None, 'ma'), may hold values from -0.1875 to 0.1875
- second_branch_tensors: bfloat16 [2, 2, 512, 512], P(None, None, 'ma'), may hold values from -0.1875 to 0.1875
- relabel: int32 [2, 512], replicated, may hold values from 0 to 511, each once within a row
- sample_block: int32 [8192, 1], P(('cuts', 'ma', 'mb')), parts along dimension 0, may hold values from 0 to 31; in each aligned block of 256 rows (0 to 255, 256 to 511, ...) at most 16 rows name the same one
- sample_state: bfloat16 [8192, 2, 512], P(('cuts', 'ma', 'mb')), parts along dimension 0, may hold values from -0.1875 to 0.1875
Outputs:
- amplitudes: bfloat16 [8192, 2, 512], P(('cuts', 'ma', 'mb')), parts along dimension 0
The draws below stay inside these ranges and needn't reach their ends.
There are 2 independent parts, one for each index of `cuts`. The reference program is written for one: setup_inputs(seed, part) draws one part's arguments, and reference() takes and returns one part's arrays. A program takes and returns all parts, laid end to end along the dimension named above; an argument that names none is the same for every part. Nothing has to cross between parts.
Inputs may be any that keep to these rules, and one draw needn't show every extreme that they name: `relabel`: each row is a permutation of 0 to 511. `sample_block`: within the 256 rows of one device no prefix block is named more than 16 times.
All inputs are finite; a program needn't handle non-finite values.
Results may differ from the reference program's by a relative error of at most 0.0075.
Values may be sent and summed in bfloat16 or wider, within the bound.
No kernel may reach another device: no remote copies, remote signals or barrier semaphores. Data moves between devices by JAX's collectives and lax.ppermute only.
A program may use at most 64 MiB of HBM per device.

```python
import math
import jax
import jax.numpy as jnp
import numpy as np
from jax import lax

FIRST_MODE_SIZE = 512
SECOND_MODE_SIZE = 512
REGROUP_COUNT = 2
SAMPLES_DEVICE = 256
S = 32
SAMP = 4096
MOST = 16
N_MA = 8
N_MB = 2


def level_of(key, extent, split, least, high):
    def one(dim, blocks):
        heights = jax.random.uniform(jax.random.fold_in(jax.random.fold_in(key, 6), dim), (blocks,), jnp.float32, least / len(split), high / len(split))
        return jnp.repeat(jnp.exp(heights), extent[dim] // blocks).reshape((-1,) + (1,) * (len(extent) - dim - 1))

    level = one(*split[0])
    for cut in split[1:]:
        level = level * one(*cut)
    return level


def shared_out(key, own, number, rows, amount, top, most, lean):
    ranking = jax.random.permutation(key, amount)
    crowded, ordinary = load_shares(amount, rows * top, most, lean, True), load_shares(amount, rows * top, most, lean, False)
    places = jnp.arange(amount)

    def named(lengths, offset_by):
        used = int((lengths > 0).sum())
        fixed = max(1, used // 4)
        passed = fixed + (places - fixed + offset_by * (used - fixed)) % max(1, amount - fixed)
        return jnp.zeros((amount,), jnp.int32).at[ranking[jnp.where(places < fixed, places, passed)]].set(jnp.asarray(lengths, jnp.int32))

    lengths = jnp.where(number % 4 == 0, named(crowded, number // 4), named(ordinary, number - number // 4 - 1))
    mixed = jax.random.permutation(jax.random.fold_in(own, 3), amount)
    source_of, sink = mixed[0:amount // 2 * 2:2], mixed[1:amount // 2 * 2:2]
    slack = jnp.minimum(lengths[source_of] - 1, most - lengths[sink]) // 2
    slack = jnp.where((source_of == ranking[0]) | (sink == ranking[0]) | (lengths[sink] == 0), 0, jnp.maximum(slack, 0))
    passed = jax.random.randint(jax.random.fold_in(own, 4), (amount // 2,), 0, 1 << 20) % (slack + 1)
    lengths = lengths.at[source_of].add(-passed).at[sink].add(passed)
    labels = jnp.searchsorted(jnp.cumsum(lengths), jnp.arange(rows * top), side="right").astype(jnp.int32)
    grid = labels.reshape(top, rows).T
    grid = grid[jax.random.permutation(jax.random.fold_in(own, 1), rows)]
    offset_by = jax.random.randint(jax.random.fold_in(own, 2), (rows, 1), 0, top)
    return jnp.take_along_axis(grid, (jnp.arange(top)[None, :] + offset_by) % top, axis=1)


def load_shares(count, total, most, lean, full):
    weights = [(1 << 20) // math.isqrt(grade ** lean) + 1 for grade in range(1, count + 1)]
    largest = most if full else min(most, max(-(-total // count), total * weights[0] // sum(weights)))
    least = 1 if total - largest >= count - 1 else 0
    given, spare = [largest] + [least] * (count - 1), total - largest - least * (count - 1)
    while spare > 0:
        candidates = [i for i in range(1, count) if given[i] < largest] or [i for i in range(1, count) if given[i] < most]
        mass, budget = sum([weights[i] for i in candidates]), spare
        for i in candidates:
            extra = min(most - given[i], max(1, budget * weights[i] // mass), spare)
            given[i] = given[i] + extra
            spare = spare - extra
    return np.array(given)


def gaussian(own_key, dims, width, limit, cuts=(), held_as=jnp.bfloat16):
    values = jax.random.normal(own_key, dims, jnp.float32) * width
    if len(cuts) > 0:
        values = level_of(own_key, dims, cuts, -0.22, 0.18) * values
    return jnp.clip(values, min=-limit, max=limit).astype(held_as)


def setup_inputs(seed: int = 0, part: int = 0) -> dict:
    keys = jax.random.split(jax.random.key(seed), 7)
    part_keys = jax.random.split(jax.random.fold_in(keys[6], part), 7)
    stem_field = gaussian(part_keys[0], (S, FIRST_MODE_SIZE, 2, SECOND_MODE_SIZE), 1.0, 6.0, ((0, 16),))
    first_branch_tensors = gaussian(keys[1], (REGROUP_COUNT, 2, FIRST_MODE_SIZE, FIRST_MODE_SIZE), (2 * FIRST_MODE_SIZE) ** -0.5, 0.1875, ((2, 8),))
    second_branch_tensors = gaussian(keys[2], (REGROUP_COUNT, 2, SECOND_MODE_SIZE, SECOND_MODE_SIZE), (2 * SECOND_MODE_SIZE) ** -0.5, 0.1875, ((2, 8),))
    relabel = jax.vmap(lambda own: jax.random.permutation(own, FIRST_MODE_SIZE))(jax.random.split(keys[3], REGROUP_COUNT)).reshape((REGROUP_COUNT, FIRST_MODE_SIZE)).astype(jnp.int32)
    sample_block_keys = jax.random.split(jax.random.fold_in(part_keys[4], 1), SAMP // SAMPLES_DEVICE)
    sample_block_turns = jax.random.permutation(jax.random.fold_in(part_keys[4], 3), SAMP // SAMPLES_DEVICE)
    sample_block = jax.vmap(lambda own, number: shared_out(jax.random.fold_in(part_keys[4], 2), own, number, SAMPLES_DEVICE, S, 1, MOST, 2))(sample_block_keys, sample_block_turns).reshape((SAMP, 1))
    sample_state = gaussian(part_keys[5], (SAMP, 2, SECOND_MODE_SIZE), (2 * SECOND_MODE_SIZE) ** -0.5, 0.1875, ((0, 16),))
    return {"stem_field": stem_field, "first_branch_tensors": first_branch_tensors, "second_branch_tensors": second_branch_tensors, "relabel": relabel, "sample_block": sample_block, "sample_state": sample_state}


def regroup(stem_field, groups):
    blocks, row_count, part_count, col_count = stem_field.shape
    local_blocks = blocks // groups
    pieces = stem_field.reshape(groups, local_blocks, groups, row_count // groups, part_count, col_count)
    pieces = jnp.transpose(pieces, (2, 1, 0, 3, 4, 5))
    return pieces.reshape(blocks, row_count, part_count, col_count)


def complex_contract(stem_field, matrix, pattern):
    real_part = stem_field[:, :, 0, :].astype(jnp.float32)
    imag_part = stem_field[:, :, 1, :].astype(jnp.float32)
    matrix_real = matrix[0].astype(jnp.float32)
    matrix_imag = matrix[1].astype(jnp.float32)

    def product(operand, table):
        return jnp.einsum(pattern, operand, table, precision=lax.Precision.HIGHEST)

    out_real = product(real_part, matrix_real) - product(imag_part, matrix_imag)
    out_imag = product(real_part, matrix_imag) + product(imag_part, matrix_real)
    return jnp.stack([out_real, out_imag], axis=2).astype(jnp.bfloat16)


def reference(stem_field, first_branch_tensors, second_branch_tensors, relabel, sample_block, sample_state):
    groups = N_MA * N_MB
    for regroup_round_index in range(REGROUP_COUNT):
        stem_field = regroup(stem_field, groups)
        stem_field = jnp.take(stem_field, relabel[regroup_round_index].astype(jnp.int32), axis=1)
        stem_field = complex_contract(stem_field, first_branch_tensors[regroup_round_index], "sab,ao->sob")
        stem_field = complex_contract(stem_field, second_branch_tensors[regroup_round_index], "sab,bo->sao")
    batch_size = 32
    owners = sample_block[:, 0].astype(jnp.int32).reshape(-1, batch_size)
    states = sample_state.reshape(-1, batch_size, 2, sample_state.shape[2])

    def evaluate(pair):
        indices, batch_states = pair
        chosen = jnp.take(stem_field, indices, axis=0).astype(jnp.float32)
        state_real = batch_states[:, 0].astype(jnp.float32)
        state_imag = batch_states[:, 1].astype(jnp.float32)

        def product(operand, vector):
            return jnp.einsum("nab,nb->na", operand, vector, precision=lax.Precision.HIGHEST)

        out_real = product(chosen[:, :, 0], state_real) - product(chosen[:, :, 1], state_imag)
        out_imag = product(chosen[:, :, 0], state_imag) + product(chosen[:, :, 1], state_real)
        return jnp.stack([out_real, out_imag], axis=1).astype(jnp.bfloat16)

    amplitudes = lax.map(evaluate, (owners, states))
    return amplitudes.reshape(sample_state.shape[0], 2, stem_field.shape[1])
```

```python
import functools

import jax
import jax.numpy as jnp
from jax import lax
from jax.experimental import pallas as pl
from jax.experimental.pallas import tpu as pltpu
from jax.sharding import PartitionSpec as P

AXES = ("ma", "mb")
BF16 = jnp.bfloat16
F32 = jnp.float32


def permute(value, pairs):
    count = lax.axis_size("mb")
    full = [(a * count + c, b * count + c) for a, b in pairs for c in range(count)]
    return lax.ppermute(value, AXES, full)


def swap_ma(value, offset):
    return permute(value, [(m, m ^ offset) for m in range(lax.axis_size("ma"))])


def swap_mb(value, offset):
    count = lax.axis_size("ma") * lax.axis_size("mb")
    return lax.ppermute(value, AXES, [(m, m ^ offset) for m in range(count)])


def relay_groups(length):
    owner, groups = {}, {}
    for distance in range(1, length):
        for z in range(length):
            for x in range(1, length):
                if abs((z ^ x) - z) != distance:
                    continue
                sender = z + (1 if (z ^ x) > z else -1)
                held = sender ^ z ^ x
                key = (x, owner.get((sender, held)))
                owner[(z, x)] = key
                groups.setdefault(key, []).append((sender, z))
    return groups


def relay_gather(value):
    length = lax.axis_size("ma") // 2
    sent = {None: value}
    slots = {0: [value]}
    for key, moves in relay_groups(length).items():
        pairs = [(2 * a + y, 2 * b + y) for a, b in moves for y in range(2)]
        sent[key] = permute(sent[key[1]], pairs)
        slots.setdefault(key[0], []).append(sent[key])
    gathered = {}
    for x in sorted(slots):
        whole = functools.reduce(jnp.add, slots[x])
        gathered[2 * x] = whole
        gathered[2 * x + 1] = swap_ma(whole, 1)
    return [gathered[d] for d in range(2 * length)]


def stem_kernel(rows_ref, table_ref, product_ref, out_ref, mid_ref):
    half = mid_ref.shape[0] // 2
    step = min(256, half)
    rows = rows_ref[0]
    for top in range(0, 2 * half, step):
        part = jnp.dot(table_ref[top : top + step, :], rows, preferred_element_type=F32)
        mid_ref[top : top + step, :] = part.astype(BF16)
    depth = mid_ref.shape[1]
    for top in range(0, half, step):
        part = jnp.dot(
            mid_ref[top : top + step, :], product_ref[:depth, :], preferred_element_type=F32
        )
        part += jnp.dot(
            mid_ref[half + top : half + top + step, :],
            product_ref[depth:, :],
            preferred_element_type=F32,
        )
        out_ref[0, top : top + step, :] = part.astype(BF16)


def contract_stem(rows, table, product):
    local, depth, width = rows.shape
    outer = table.shape[0] // 2
    return pl.pallas_call(
        stem_kernel,
        grid=(local,),
        in_specs=[
            pl.BlockSpec((1, depth, width), lambda l: (l, 0, 0)),
            pl.BlockSpec(table.shape, lambda l: (0, 0)),
            pl.BlockSpec(product.shape, lambda l: (0, 0)),
        ],
        out_specs=pl.BlockSpec((1, outer, 2 * width), lambda l: (l, 0, 0)),
        out_shape=jax.ShapeDtypeStruct((local, outer, 2 * width), BF16),
        scratch_shapes=[pltpu.VMEM((2 * outer, width), BF16)],
        cost_estimate=pl.CostEstimate(
            flops=2 * local * (2 * outer * depth * width + outer * 4 * width * width),
            bytes_accessed=2 * (2 * rows.size + table.size + product.size),
            transcendentals=0,
        ),
        name="contract_stem",
    )(rows, table, product)


def sample_kernel(groups, state_ref, *refs):
    stems, (out_ref, plus_ref, cross_ref, sum_ref) = refs[:-4], refs[-4:]
    block, last = pl.program_id(1), pl.num_programs(1) - 1
    depth = plus_ref.shape[0]
    width = depth // 2

    @pl.when(block == 0)
    def _():
        plus_ref[:width, :] = state_ref[0, :width, :]
        plus_ref[width:, :] = -state_ref[0, width:depth, :]
        cross_ref[:width, :] = state_ref[0, width:depth, :]
        cross_ref[width:, :] = state_ref[0, :width, :]
        sum_ref[...] = jnp.zeros_like(sum_ref)

    named = state_ref[0, depth : depth + 16, :].astype(F32)[:1, :]
    local = pl.num_programs(1)
    for s, stem_ref in enumerate(stems):
        rows = stem_ref.shape[1]
        inner = rows // groups
        step = min(256, rows)
        for part, weights in enumerate((plus_ref, cross_ref)):
            total = sum_ref[s, part]
            for top in range(0, rows, step):
                value = jnp.dot(
                    stem_ref[0, top : top + step, :], weights[...], preferred_element_type=F32
                )
                for k in range(step // inner):
                    number = ((top // inner + k) * local + block).astype(F32)
                    total += jnp.where(named == number, value[k * inner : (k + 1) * inner, :], 0.0)
            sum_ref[s, part] = total

    @pl.when(block == last)
    def _():
        out_ref[0] = sum_ref[...].astype(BF16)


def contract_samples(states, stems, groups):
    many, depth, samples = states.shape
    local, rows, width = stems[0].shape
    inner = rows // groups
    out = (len(stems), 2, inner, samples)
    return pl.pallas_call(
        functools.partial(sample_kernel, groups),
        grid=(many, local),
        in_specs=[pl.BlockSpec((1, depth, samples), lambda m, l: (m, 0, 0))]
        + [pl.BlockSpec((1, rows, width), lambda m, l: (l, 0, 0))] * len(stems),
        out_specs=pl.BlockSpec((1,) + out, lambda m, l: (m, 0, 0, 0, 0)),
        out_shape=jax.ShapeDtypeStruct((many,) + out, BF16),
        scratch_shapes=[
            pltpu.VMEM((width, samples), BF16),
            pltpu.VMEM((width, samples), BF16),
            pltpu.VMEM(out, F32),
        ],
        cost_estimate=pl.CostEstimate(
            flops=2 * many * local * rows * width * 2 * samples * len(stems),
            bytes_accessed=2 * (states.size + len(stems) * stems[0].size),
            transcendentals=0,
        ),
        name="contract_samples",
    )(states, *stems)


def first_table(tensor, relabel, places):
    selector = (relabel[:, None] == places[None, :]).astype(BF16)
    ordered = jnp.einsum("pio,iq->poq", tensor, selector, preferred_element_type=F32).astype(BF16)
    upper = jnp.concatenate([ordered[0], -ordered[1]], axis=1)
    lower = jnp.concatenate([ordered[1], ordered[0]], axis=1)
    return jnp.concatenate([upper, lower], axis=0)


def second_product(tensors):
    left = tensors[0]
    for right in [tensors[r] for r in range(1, tensors.shape[0])]:
        rows = jnp.concatenate([left[0], left[1]], axis=1)
        upper = jnp.concatenate([right[0], right[1]], axis=1)
        lower = jnp.concatenate([-right[1], right[0]], axis=1)
        table = jnp.concatenate([upper, lower], axis=0)
        both = jnp.dot(rows, table, preferred_element_type=F32).astype(BF16)
        width = right.shape[2]
        left = jnp.stack([both[:, :width], both[:, width:]])
    upper = jnp.concatenate([left[0], left[1]], axis=1)
    lower = jnp.concatenate([-left[1], left[0]], axis=1)
    return jnp.concatenate([upper, lower], axis=0)


def on_device(
    stem_field, first_branch_tensors, second_branch_tensors, relabel, sample_block, sample_state
):
    count_ma, count_mb = lax.axis_size("ma"), lax.axis_size("mb")
    here_ma, here_mb = lax.axis_index("ma"), lax.axis_index("mb")
    groups = count_ma * count_mb
    local, row_count, parts, width = stem_field.shape
    inner = row_count // groups
    samples = sample_state.shape[0]
    short = count_ma // 2 <= 4
    slots = jnp.arange(count_ma, dtype=jnp.int32)
    seats = jnp.arange(count_mb, dtype=jnp.int32)
    near_ma = slots ^ here_ma if short else slots
    near_mb = seats ^ here_mb

    def places(ma_of, mb_of):
        base = (ma_of[:, None] * count_mb + mb_of[None, :]).reshape(-1) * inner
        return (base[:, None] + jnp.arange(inner, dtype=jnp.int32)[None, :]).reshape(-1)

    flat = sample_state.reshape(samples, parts * width).T
    named = jnp.broadcast_to(sample_block[:, 0].astype(BF16)[None, :], (16, samples))
    states = jnp.concatenate([flat, named], axis=0)

    pieces = stem_field.reshape(local, count_ma, count_mb, inner, parts, width)
    pieces = jnp.transpose(pieces, (2, 1, 4, 0, 3, 5))

    if short:
        share = jnp.where(here_mb == 0, first_branch_tensors, second_branch_tensors)
        branch = relay_gather(share)
        stacked = jnp.stack(branch)
        natural = jnp.concatenate(
            [lax.dynamic_index_in_dim(stacked, m ^ here_ma, keepdims=False) for m in range(count_ma)],
            axis=2,
        )
        other = swap_mb(natural, 1)
        every_first = jnp.where(here_mb == 0, natural, other)
        every_second = jnp.where(here_mb == 0, other, natural)

        mine = [
            lax.dynamic_index_in_dim(pieces, here_mb ^ s, keepdims=False) for s in range(count_mb)
        ]
        chip = jnp.stack([mine[0]] + [swap_mb(mine[s], s) for s in range(1, count_mb)])
        arrived = []
        for d in range(count_ma):
            piece = lax.dynamic_index_in_dim(chip, here_ma ^ d, 1, keepdims=False)
            arrived.append(swap_ma(piece, d) if d else piece)
        rows = jnp.stack(arrived)
        rows = jnp.transpose(rows, (3, 2, 0, 1, 4, 5)).reshape(local, parts * row_count, width)
        first_places = places(near_ma, near_mb)
        every_state = relay_gather(states)
    else:
        every_first = lax.all_gather(first_branch_tensors, "ma", axis=2, tiled=True)
        every_second = lax.all_gather(second_branch_tensors, "ma", axis=2, tiled=True)
        sent = jnp.transpose(pieces, (1, 0, 2, 3, 4, 5)).reshape(
            groups, parts, local, inner, width
        )
        rows = lax.all_to_all(sent, AXES, split_axis=0, concat_axis=0, tiled=True)
        rows = jnp.transpose(rows, (2, 1, 0, 3, 4)).reshape(local, parts * row_count, width)
        first_places = places(slots, seats)
        every_state = lax.all_gather(states, "ma", axis=0)

    table = first_table(every_first[0], relabel[0], first_places)
    final_table = first_table(every_first[1], relabel[1], places(near_ma, near_mb))
    product = second_product(every_second)
    own = contract_stem(rows, table, product)
    stems = [own] + [swap_mb(own, s) for s in range(1, count_mb)]
    if short:
        found = []
        for d in range(count_ma):
            value = contract_samples(every_state[d][None], stems, groups)[0]
            found.append(swap_ma(value, d) if d else value)
        found = jnp.stack(found)
    else:
        value = contract_samples(every_state, stems, groups)
        found = lax.all_to_all(value, "ma", split_axis=0, concat_axis=0, tiled=True)
    found = jnp.transpose(found, (2, 0, 1, 3, 4)).reshape(parts * row_count, samples)
    amplitudes = jnp.einsum("kn,mk->nm", found, final_table, preferred_element_type=F32)
    return amplitudes.astype(BF16).reshape(samples, parts, -1)


def solution(mesh):
    placed = (
        P(("cuts", "ma", "mb"), None, None, None),
        P(None, None, "ma", None),
        P(None, None, "ma", None),
        P(),
        P(("cuts", "ma", "mb"), None),
        P(("cuts", "ma", "mb"), None, None),
    )
    return jax.shard_map(
        on_device,
        mesh=mesh,
        in_specs=placed,
        out_specs=P(("cuts", "ma", "mb"), None, None),
        check_vma=False,
    )
```

```python
import functools

import jax
import jax.numpy as jnp
from jax import lax
from jax.experimental import pallas as pl
from jax.experimental.pallas import tpu as pltpu
from jax.sharding import PartitionSpec as P

AXES = ("ma", "mb")
BF16 = jnp.bfloat16
F32 = jnp.float32
VMEM = pl.BlockSpec(memory_space=pltpu.VMEM)
SMEM = pl.BlockSpec(memory_space=pltpu.SMEM)


def permute(value, pairs):
    count = lax.axis_size("mb")
    full = [(a * count + c, b * count + c) for a, b in pairs for c in range(count)]
    return lax.ppermute(value, AXES, full)


def swap_ma(value, offset):
    return permute(value, [(m, m ^ offset) for m in range(lax.axis_size("ma"))])


def swap_mb(value, offset):
    count = lax.axis_size("ma") * lax.axis_size("mb")
    return lax.ppermute(value, AXES, [(m, m ^ offset) for m in range(count)])


def relay_groups(length):
    owner, groups = {}, {}
    for distance in range(1, length):
        for z in range(length):
            for x in range(1, length):
                if abs((z ^ x) - z) != distance:
                    continue
                sender = z + (1 if (z ^ x) > z else -1)
                held = sender ^ z ^ x
                key = (x, owner.get((sender, held)))
                owner[(z, x)] = key
                groups.setdefault(key, []).append((sender, z))
    return groups


def relay_gather(value):
    length = lax.axis_size("ma") // 2
    sent = {None: value}
    slots = {0: [value]}
    for key, moves in relay_groups(length).items():
        pairs = [(2 * a + y, 2 * b + y) for a, b in moves for y in range(2)]
        sent[key] = permute(sent[key[1]], pairs)
        slots.setdefault(key[0], []).append(sent[key])
    gathered = {}
    for x in sorted(slots):
        whole = functools.reduce(jnp.add, slots[x])
        gathered[2 * x] = whole
        gathered[2 * x + 1] = swap_ma(whole, 1)
    return [gathered[d] for d in range(2 * length)]


def scalars(*values):
    return jnp.stack([jnp.asarray(v, jnp.int32) for v in values])


def pack_kernel(place_ref, *refs):
    count = refs[0].shape[0]
    sources, outs = refs[:-count], refs[-count:]
    for d, out_ref in enumerate(outs):
        for s, source in enumerate(sources):
            out_ref[s] = source[place_ref[0] ^ d]


def pack(here_ma, sources):
    count = sources[0].shape[0]
    shape = (len(sources),) + sources[0].shape[1:]
    return pl.pallas_call(
        pack_kernel,
        in_specs=[SMEM] + [VMEM] * len(sources),
        out_specs=[VMEM] * count,
        out_shape=[jax.ShapeDtypeStruct(shape, BF16)] * count,
        name="pack",
    )(scalars(here_ma), *sources)


def collect_kernel(place_ref, *refs):
    slots, out_ref = refs[:-1], refs[-1]
    depth = slots[0].shape[2]
    for d, slot in enumerate(slots):
        start = pl.multiple_of((place_ref[0] ^ d) * depth, depth)
        out_ref[:, :, pl.ds(start, depth), :] = slot[...]


def collect(here_ma, slots):
    rounds, parts, depth, width = slots[0].shape
    return pl.pallas_call(
        collect_kernel,
        in_specs=[SMEM] + [VMEM] * len(slots),
        out_specs=VMEM,
        out_shape=jax.ShapeDtypeStruct((rounds, parts, depth * len(slots), width), BF16),
        name="collect",
    )(scalars(here_ma), *slots)


def table_kernel(inner, count_mb, relative, place_ref, relabel_ref, first_ref, second_ref, *refs):
    stem_ref, final_ref, product_ref, right_ref = refs
    size = first_ref.shape[2]
    column = lax.broadcasted_iota(jnp.int32, (size, size), 0)
    seat, rest = column // inner, column % inner
    ma, mb = seat // count_mb, seat % count_mb
    near = (((ma ^ place_ref[0]) * count_mb) + (mb ^ place_ref[1])) * inner + rest
    for r in range(2):
        position = near if relative[r] else column
        selector = jnp.where(relabel_ref[r : r + 1, :] == position, 1.0, 0.0).astype(BF16)
        for p in range(2):
            ordered = jnp.dot(selector, first_ref[r, p], preferred_element_type=F32)
            if r == 0:
                turned = ordered.T.astype(BF16)
                if p == 0:
                    stem_ref[:size, :size] = turned
                    stem_ref[size:, size:] = turned
                else:
                    stem_ref[size:, :size] = turned
                    stem_ref[:size, size:] = -turned
            else:
                ordered = ordered.astype(BF16)
                if p == 0:
                    final_ref[:size, :size] = ordered
                    final_ref[size:, size:] = ordered
                else:
                    final_ref[:size, size:] = ordered
                    final_ref[size:, :size] = -ordered
    width = second_ref.shape[2]
    right_ref[:width, :width] = second_ref[1, 0]
    right_ref[:width, width:] = second_ref[1, 1]
    right_ref[width:, :width] = -second_ref[1, 1]
    right_ref[width:, width:] = second_ref[1, 0]
    both = jnp.dot(second_ref[0, 0], right_ref[:width, :], preferred_element_type=F32)
    both += jnp.dot(second_ref[0, 1], right_ref[width:, :], preferred_element_type=F32)
    both = both.astype(BF16)
    product_ref[:width, :] = both
    product_ref[width:, :width] = -both[:, width:]
    product_ref[width:, width:] = both[:, :width]


def tables(here, relabel, first, second, inner, count_mb, relative):
    size, width = 2 * first.shape[2], 2 * second.shape[2]
    return pl.pallas_call(
        functools.partial(table_kernel, inner, count_mb, relative),
        in_specs=[SMEM] + [VMEM] * 3,
        out_specs=[VMEM] * 3,
        out_shape=[
            jax.ShapeDtypeStruct((size, size), BF16),
            jax.ShapeDtypeStruct((size, size), BF16),
            jax.ShapeDtypeStruct((width, width), BF16),
        ],
        scratch_shapes=[pltpu.VMEM((width, width), BF16)],
        cost_estimate=pl.CostEstimate(
            flops=size**3 + width**3, bytes_accessed=10 * size * size, transcendentals=0
        ),
        name="tables",
    )(here, relabel, first, second)


def stem_kernel(*refs):
    arrived, (table_ref, product_ref, out_ref, rows_ref, mid_ref) = refs[:-5], refs[-5:]
    seats, parts, _, inner, _ = arrived[0].shape
    for d, piece in enumerate(arrived):
        for s in range(seats):
            for p in range(parts):
                start = ((p * len(arrived) + d) * seats + s) * inner
                rows_ref[start : start + inner, :] = piece[s, p, 0]
    half = mid_ref.shape[0] // 2
    step = min(256, half)
    for top in range(0, 2 * half, step):
        part = jnp.dot(table_ref[top : top + step, :], rows_ref[...], preferred_element_type=F32)
        mid_ref[top : top + step, :] = part.astype(BF16)
    depth = mid_ref.shape[1]
    for top in range(0, half, step):
        part = jnp.dot(
            mid_ref[top : top + step, :], product_ref[:depth, :], preferred_element_type=F32
        )
        part += jnp.dot(
            mid_ref[half + top : half + top + step, :],
            product_ref[depth:, :],
            preferred_element_type=F32,
        )
        out_ref[0, top : top + step, :] = part.astype(BF16)


def contract_stem(arrived, table, product):
    seats, parts, local, inner, width = arrived[0].shape
    size = table.shape[0]
    piece = pl.BlockSpec((seats, parts, 1, inner, width), lambda l: (0, 0, l, 0, 0))
    return pl.pallas_call(
        stem_kernel,
        grid=(local,),
        in_specs=[piece] * len(arrived)
        + [
            pl.BlockSpec(table.shape, lambda l: (0, 0)),
            pl.BlockSpec(product.shape, lambda l: (0, 0)),
        ],
        out_specs=pl.BlockSpec((1, size // 2, 2 * width), lambda l: (l, 0, 0)),
        out_shape=jax.ShapeDtypeStruct((local, size // 2, 2 * width), BF16),
        scratch_shapes=[pltpu.VMEM((size, width), BF16), pltpu.VMEM((size, width), BF16)],
        cost_estimate=pl.CostEstimate(
            flops=2 * local * (size * size * width + 2 * size * width * width),
            bytes_accessed=4 * (local * size * width + table.size),
            transcendentals=0,
        ),
        name="contract_stem",
    )(*arrived, table, product)


def sample_kernel(groups, many, *refs):
    states, refs = refs[:many], refs[many:]
    outs, (plus_ref, cross_ref, sum_ref) = refs[-3 - many : -3], refs[-3:]
    stems = refs[: -3 - many]
    block, last = pl.program_id(0), pl.num_programs(0) - 1
    depth = plus_ref.shape[1]
    width = depth // 2

    @pl.when(block == 0)
    def _():
        for m, state_ref in enumerate(states):
            plus_ref[m, :width, :] = state_ref[:width, :]
            plus_ref[m, width:, :] = -state_ref[width:depth, :]
            cross_ref[m, :width, :] = state_ref[width:depth, :]
            cross_ref[m, width:, :] = state_ref[:width, :]
        sum_ref[...] = jnp.zeros_like(sum_ref)

    local = pl.num_programs(0)
    for m, state_ref in enumerate(states):
        named = state_ref[depth : depth + 16, :].astype(F32)[:1, :]
        for s, stem_ref in enumerate(stems):
            rows = stem_ref.shape[1]
            inner = rows // groups
            step = min(256, rows)
            for part, weights in enumerate((plus_ref, cross_ref)):
                total = sum_ref[m, s, part]
                for top in range(0, rows, step):
                    value = jnp.dot(
                        stem_ref[0, top : top + step, :], weights[m], preferred_element_type=F32
                    )
                    for k in range(step // inner):
                        number = ((top // inner + k) * local + block).astype(F32)
                        part_of = value[k * inner : (k + 1) * inner, :]
                        total += jnp.where(named == number, part_of, 0.0)
                sum_ref[m, s, part] = total

    @pl.when(block == last)
    def _():
        for m, out_ref in enumerate(outs):
            out_ref[...] = sum_ref[m].astype(BF16)


def contract_samples(states, stems, groups):
    many = len(states)
    depth, samples = states[0].shape
    local, rows, width = stems[0].shape
    out = (len(stems), 2, rows // groups, samples)
    return pl.pallas_call(
        functools.partial(sample_kernel, groups, many),
        grid=(local,),
        in_specs=[pl.BlockSpec((depth, samples), lambda l: (0, 0))] * many
        + [pl.BlockSpec((1, rows, width), lambda l: (l, 0, 0))] * len(stems),
        out_specs=[pl.BlockSpec(out, lambda l: (0, 0, 0, 0))] * many,
        out_shape=[jax.ShapeDtypeStruct(out, BF16)] * many,
        scratch_shapes=[
            pltpu.VMEM((many, width, samples), BF16),
            pltpu.VMEM((many, width, samples), BF16),
            pltpu.VMEM((many,) + out, F32),
        ],
        cost_estimate=pl.CostEstimate(
            flops=2 * many * local * rows * width * 2 * samples * len(stems),
            bytes_accessed=2 * (many * states[0].size + len(stems) * stems[0].size),
            transcendentals=0,
        ),
        name="contract_samples",
    )(*states, *stems)


def final_kernel(*refs):
    found, (table_ref, out_ref, rows_ref) = refs[:-3], refs[-3:]
    seats, parts, inner, _ = found[0].shape
    for d, piece in enumerate(found):
        for s in range(seats):
            for p in range(parts):
                start = ((p * len(found) + d) * seats + s) * inner
                rows_ref[start : start + inner, :] = piece[s, p]
    out_ref[...] = lax.dot_general(
        rows_ref[...], table_ref[...], (((0,), (0,)), ((), ())), preferred_element_type=F32
    ).astype(BF16)


def contract_final(found, table):
    samples = found[0].shape[3]
    return pl.pallas_call(
        final_kernel,
        in_specs=[VMEM] * (len(found) + 1),
        out_specs=VMEM,
        out_shape=jax.ShapeDtypeStruct((samples, table.shape[1]), BF16),
        scratch_shapes=[pltpu.VMEM((table.shape[0], samples), BF16)],
        cost_estimate=pl.CostEstimate(
            flops=2 * table.size * samples, bytes_accessed=2 * table.size, transcendentals=0
        ),
        name="contract_final",
    )(*found, table)


def is_short(count_ma):
    return count_ma // 2 <= 4


def on_device(
    stem_field, first_branch_tensors, second_branch_tensors, relabel, sample_block, sample_state
):
    count_ma, count_mb = lax.axis_size("ma"), lax.axis_size("mb")
    here_ma, here_mb = lax.axis_index("ma"), lax.axis_index("mb")
    groups = count_ma * count_mb
    local, row_count, parts, width = stem_field.shape
    inner = row_count // groups
    samples = sample_state.shape[0]
    short = is_short(count_ma)

    flat = sample_state.reshape(samples, parts * width).T
    named = jnp.broadcast_to(sample_block[:, 0].astype(BF16)[None, :], (16, samples))
    states = jnp.concatenate([flat, named], axis=0)

    pieces = stem_field.reshape(local, count_ma, count_mb, inner, parts, width)
    pieces = jnp.transpose(pieces, (2, 1, 4, 0, 3, 5))

    if short:
        share = jnp.where(here_mb == 0, first_branch_tensors, second_branch_tensors)
        mine = collect(here_ma, relay_gather(share))
        other = swap_mb(mine, 1)
        every_first = jnp.where(here_mb == 0, mine, other)
        every_second = jnp.where(here_mb == 0, other, mine)
        held = [
            lax.dynamic_index_in_dim(pieces, here_mb ^ s, keepdims=False) for s in range(count_mb)
        ]
        sources = [held[0]] + [swap_mb(held[s], s) for s in range(1, count_mb)]
        arrived = [
            swap_ma(piece, d) if d else piece
            for d, piece in enumerate(pack(here_ma, sources))
        ]
        every_state = relay_gather(states)
    else:
        every_first = lax.all_gather(first_branch_tensors, "ma", axis=2, tiled=True)
        every_second = lax.all_gather(second_branch_tensors, "ma", axis=2, tiled=True)
        sent = jnp.transpose(pieces, (1, 0, 2, 3, 4, 5))
        sent = sent.reshape((groups,) + sent.shape[2:])
        arrived = lax.all_to_all(sent, AXES, split_axis=0, concat_axis=0, tiled=True)
        arrived = arrived.reshape((count_ma, count_mb) + arrived.shape[1:])
        arrived = [arrived[d] for d in range(count_ma)]
        every_state = lax.all_gather(states, "ma", axis=0)
        every_state = [every_state[d] for d in range(count_ma)]

    here = scalars(here_ma if short else 0, here_mb)
    table, final_table, product = tables(
        here, relabel, every_first, every_second, inner, count_mb, (short, True)
    )
    own = contract_stem(arrived, table, product)
    stems = [own] + [swap_mb(own, s) for s in range(1, count_mb)]
    found = []
    for d in range(0, count_ma, 2):
        found += contract_samples(every_state[d : d + 2], stems, groups)
    if short:
        found = [swap_ma(value, d) if d else value for d, value in enumerate(found)]
    else:
        found = lax.all_to_all(jnp.stack(found), "ma", split_axis=0, concat_axis=0, tiled=True)
        found = [found[d] for d in range(count_ma)]
    return contract_final(found, final_table).reshape(samples, parts, -1)


def solution(mesh):
    placed = (
        P(("cuts", "ma", "mb"), None, None, None),
        P(None, None, "ma", None),
        P(None, None, "ma", None),
        P(),
        P(("cuts", "ma", "mb"), None),
        P(("cuts", "ma", "mb"), None, None),
    )
    return jax.shard_map(
        on_device,
        mesh=mesh,
        in_specs=placed,
        out_specs=P(("cuts", "ma", "mb"), None, None),
        check_vma=False,
    )
```

```python
import functools

import jax
import jax.numpy as jnp
from jax import lax
from jax.experimental import pallas as pl
from jax.experimental.pallas import tpu as pltpu
from jax.sharding import PartitionSpec as P

AXES = ("ma", "mb")
BF16 = jnp.bfloat16
F32 = jnp.float32
VMEM = pl.BlockSpec(memory_space=pltpu.VMEM)
SMEM = pl.BlockSpec(memory_space=pltpu.SMEM)

LIMIT = 24 * 1024 * 1024


def params():
    return pltpu.CompilerParams(vmem_limit_bytes=LIMIT)


def permute(value, pairs):
    count = lax.axis_size("mb")
    full = [(a * count + c, b * count + c) for a, b in pairs for c in range(count)]
    return lax.ppermute(value, AXES, full)


def swap_ma(value, offset):
    return permute(value, [(m, m ^ offset) for m in range(lax.axis_size("ma"))])


def swap_mb(value, offset):
    count = lax.axis_size("ma") * lax.axis_size("mb")
    return lax.ppermute(value, AXES, [(m, m ^ offset) for m in range(count)])


def relay_groups(length):
    owner, groups = {}, {}
    for distance in range(1, length):
        for z in range(length):
            for x in range(1, length):
                if abs((z ^ x) - z) != distance:
                    continue
                sender = z + (1 if (z ^ x) > z else -1)
                held = sender ^ z ^ x
                key = (x, owner.get((sender, held)))
                owner[(z, x)] = key
                groups.setdefault(key, []).append((sender, z))
    return groups


def relay_gather(value):
    length = lax.axis_size("ma") // 2
    sent = {None: value}
    slots = {0: [value]}
    for key, moves in relay_groups(length).items():
        pairs = [(2 * a + y, 2 * b + y) for a, b in moves for y in range(2)]
        sent[key] = permute(sent[key[1]], pairs)
        slots.setdefault(key[0], []).append(sent[key])
    gathered = {}
    for x in sorted(slots):
        whole = functools.reduce(jnp.add, slots[x])
        gathered[2 * x] = whole
        gathered[2 * x + 1] = swap_ma(whole, 1)
    return [gathered[d] for d in range(2 * length)]


def scalars(*values):
    return jnp.stack([jnp.asarray(v, jnp.int32) for v in values])


def pack_kernel(count, place_ref, *refs):
    sources, outs = refs[: -count * refs[0].shape[2]], refs[-count * refs[0].shape[2] :]
    for number, out_ref in enumerate(outs):
        l, d = number // count, number % count
        for s, source in enumerate(sources):
            out_ref[s] = source[place_ref[0] ^ d, :, l]


def pack(here_ma, sources):
    count, parts, local, inner, width = sources[0].shape
    shape = jax.ShapeDtypeStruct((len(sources), parts, inner, width), BF16)
    outs = pl.pallas_call(
        functools.partial(pack_kernel, count),
        in_specs=[SMEM] + [VMEM] * len(sources),
        out_specs=[VMEM] * (count * local),
        out_shape=[shape] * (count * local),
        compiler_params=params(),
        name="pack",
    )(scalars(here_ma), *sources)
    return [outs[l * count : (l + 1) * count] for l in range(local)]


def table_kernel(inner, count_mb, relative, slots, place_ref, relabel_ref, *refs):
    mine, other, refs = refs[:slots], refs[slots : 2 * slots], refs[2 * slots :]
    stem_ref, final_ref, product_ref, first_ref, second_ref, right_ref = refs
    depth = mine[0].shape[2]

    def gather(first, second):
        for d in range(slots):
            start = pl.multiple_of((place_ref[2] ^ d) * depth, depth)
            first_ref[:, :, pl.ds(start, depth), :] = first[d][...]
            second_ref[:, :, pl.ds(start, depth), :] = second[d][...]

    @pl.when(place_ref[3] == 0)
    def _():
        gather(mine, other)

    @pl.when(place_ref[3] != 0)
    def _():
        gather(other, mine)

    size = first_ref.shape[2]
    column = lax.broadcasted_iota(jnp.int32, (size, size), 0)
    seat, rest = column // inner, column % inner
    ma, mb = seat // count_mb, seat % count_mb
    near = (((ma ^ place_ref[0]) * count_mb) + (mb ^ place_ref[1])) * inner + rest
    for r in range(2):
        position = near if relative[r] else column
        selector = jnp.where(relabel_ref[r : r + 1, :] == position, 1.0, 0.0).astype(BF16)
        for p in range(2):
            ordered = jnp.dot(selector, first_ref[r, p], preferred_element_type=F32)
            if r == 0:
                turned = ordered.T.astype(BF16)
                if p == 0:
                    stem_ref[:size, :size] = turned
                    stem_ref[size:, size:] = turned
                else:
                    stem_ref[size:, :size] = turned
                    stem_ref[:size, size:] = -turned
            else:
                ordered = ordered.astype(BF16)
                if p == 0:
                    final_ref[:size, :size] = ordered
                    final_ref[size:, size:] = ordered
                else:
                    final_ref[:size, size:] = ordered
                    final_ref[size:, :size] = -ordered
    width = second_ref.shape[2]
    right_ref[:width, :width] = second_ref[1, 0]
    right_ref[:width, width:] = second_ref[1, 1]
    right_ref[width:, :width] = -second_ref[1, 1]
    right_ref[width:, width:] = second_ref[1, 0]
    both = jnp.dot(second_ref[0, 0], right_ref[:width, :], preferred_element_type=F32)
    both += jnp.dot(second_ref[0, 1], right_ref[width:, :], preferred_element_type=F32)
    both = both.astype(BF16)
    product_ref[:width, :] = both
    product_ref[width:, :width] = -both[:, width:]
    product_ref[width:, width:] = both[:, :width]


def tables(here, relabel, mine, other, inner, count_mb, relative):
    rounds, parts, depth, width = mine[0].shape
    size = depth * len(mine)
    tensors = pltpu.VMEM((rounds, parts, size, width), BF16)
    return pl.pallas_call(
        functools.partial(table_kernel, inner, count_mb, relative, len(mine)),
        in_specs=[SMEM] + [VMEM] * (1 + 2 * len(mine)),
        out_specs=[VMEM] * 3,
        out_shape=[jax.ShapeDtypeStruct((2 * size, 2 * size), BF16)] * 3,
        scratch_shapes=[tensors, tensors, pltpu.VMEM((2 * size, 2 * size), BF16)],
        cost_estimate=pl.CostEstimate(
            flops=16 * size**3, bytes_accessed=40 * size * size, transcendentals=0
        ),
        compiler_params=params(),
        name="tables",
    )(here, relabel, *mine, *other)


def stem_kernel(*refs):
    arrived, (table_ref, product_ref, out_ref, rows_ref, mid_ref) = refs[:-5], refs[-5:]
    seats, parts, inner, _ = arrived[0].shape
    for d, piece in enumerate(arrived):
        for s in range(seats):
            for p in range(parts):
                start = ((p * len(arrived) + d) * seats + s) * inner
                rows_ref[start : start + inner, :] = piece[s, p]
    half = mid_ref.shape[0] // 2
    step = min(256, half)
    for top in range(0, 2 * half, step):
        part = jnp.dot(table_ref[top : top + step, :], rows_ref[...], preferred_element_type=F32)
        mid_ref[top : top + step, :] = part.astype(BF16)
    depth = mid_ref.shape[1]
    for top in range(0, half, step):
        part = jnp.dot(
            mid_ref[top : top + step, :], product_ref[:depth, :], preferred_element_type=F32
        )
        part += jnp.dot(
            mid_ref[half + top : half + top + step, :],
            product_ref[depth:, :],
            preferred_element_type=F32,
        )
        out_ref[top : top + step, :] = part.astype(BF16)


def contract_stem(arrived, table, product):
    width = arrived[0].shape[3]
    size = table.shape[0]
    return pl.pallas_call(
        stem_kernel,
        in_specs=[VMEM] * (len(arrived) + 2),
        out_specs=VMEM,
        out_shape=jax.ShapeDtypeStruct((size // 2, 2 * width), BF16),
        scratch_shapes=[pltpu.VMEM((size, width), BF16), pltpu.VMEM((size, width), BF16)],
        cost_estimate=pl.CostEstimate(
            flops=2 * (size * size * width + 2 * size * width * width),
            bytes_accessed=4 * (size * width + table.size),
            transcendentals=0,
        ),
        compiler_params=params(),
        name="contract_stem",
    )(*arrived, table, product)


def sample_kernel(groups, first, scale, many, seats, *refs):
    states, stems, refs = refs[:many], refs[many : many + seats], refs[many + seats :]
    before, outs = refs[: -2 - many], refs[-2 - many : -2]
    plus_ref, cross_ref = refs[-2:]
    depth = plus_ref.shape[0]
    width = depth // 2
    rows = stems[0].shape[0]
    inner = rows // groups
    step = min(256, rows)
    for m, state_ref in enumerate(states):
        plus_ref[:width, :] = state_ref[:width, :]
        plus_ref[width:, :] = -state_ref[width:depth, :]
        cross_ref[:width, :] = state_ref[width:depth, :]
        cross_ref[width:, :] = state_ref[:width, :]
        named = state_ref[depth : depth + 16, :].astype(F32)[:1, :]
        for s, stem_ref in enumerate(stems):
            for part, weights in enumerate((plus_ref, cross_ref)):
                total = before[m][s, part].astype(F32) if before else 0.0
                for top in range(0, rows, step):
                    value = jnp.dot(
                        stem_ref[top : top + step, :], weights[...], preferred_element_type=F32
                    )
                    for k in range(step // inner):
                        number = float((top // inner + k) * scale + first)
                        part_of = value[k * inner : (k + 1) * inner, :]
                        total += jnp.where(named == number, part_of, 0.0)
                outs[m][s, part] = total.astype(BF16)


def contract_samples(states, stems, groups, first, scale, before):
    many, seats = len(states), len(stems)
    _, samples = states[0].shape
    rows, width = stems[0].shape
    out = (seats, 2, rows // groups, samples)
    return pl.pallas_call(
        functools.partial(sample_kernel, groups, first, scale, many, seats),
        in_specs=[VMEM] * (many + seats + len(before)),
        out_specs=[VMEM] * many,
        out_shape=[jax.ShapeDtypeStruct(out, BF16)] * many,
        scratch_shapes=[pltpu.VMEM((width, samples), BF16)] * 2,
        cost_estimate=pl.CostEstimate(
            flops=2 * many * rows * width * 2 * samples * seats,
            bytes_accessed=2 * (many * states[0].size + seats * stems[0].size),
            transcendentals=0,
        ),
        compiler_params=params(),
        name="contract_samples",
    )(*states, *stems, *before)


def final_kernel(*refs):
    found, (table_ref, out_ref, rows_ref) = refs[:-3], refs[-3:]
    seats, parts, inner, _ = found[0].shape
    for d, piece in enumerate(found):
        for s in range(seats):
            for p in range(parts):
                start = ((p * len(found) + d) * seats + s) * inner
                rows_ref[start : start + inner, :] = piece[s, p]
    out_ref[...] = lax.dot_general(
        rows_ref[...], table_ref[...], (((0,), (0,)), ((), ())), preferred_element_type=F32
    ).astype(BF16)


def contract_final(found, table):
    samples = found[0].shape[3]
    return pl.pallas_call(
        final_kernel,
        in_specs=[VMEM] * (len(found) + 1),
        out_specs=VMEM,
        out_shape=jax.ShapeDtypeStruct((samples, table.shape[1]), BF16),
        scratch_shapes=[pltpu.VMEM((table.shape[0], samples), BF16)],
        cost_estimate=pl.CostEstimate(
            flops=2 * table.size * samples, bytes_accessed=2 * table.size, transcendentals=0
        ),
        compiler_params=params(),
        name="contract_final",
    )(*found, table)


def is_short(count_ma):
    return count_ma // 2 <= 4


def on_device(
    stem_field, first_branch_tensors, second_branch_tensors, relabel, sample_block, sample_state
):
    count_ma, count_mb = lax.axis_size("ma"), lax.axis_size("mb")
    here_ma, here_mb = lax.axis_index("ma"), lax.axis_index("mb")
    groups = count_ma * count_mb
    local, row_count, parts, width = stem_field.shape
    inner = row_count // groups
    samples = sample_state.shape[0]
    short = is_short(count_ma)

    flat = sample_state.reshape(samples, parts * width).T
    named = jnp.broadcast_to(sample_block[:, 0].astype(BF16)[None, :], (16, samples))
    states = jnp.concatenate([flat, named], axis=0)

    pieces = stem_field.reshape(local, count_ma, count_mb, inner, parts, width)
    pieces = jnp.transpose(pieces, (2, 1, 4, 0, 3, 5))

    if short:
        share = jnp.where(here_mb == 0, first_branch_tensors, second_branch_tensors)
        mine = relay_gather(share)
        other = [swap_mb(value, 1) for value in mine]
        held = [
            lax.dynamic_index_in_dim(pieces, here_mb ^ s, keepdims=False) for s in range(count_mb)
        ]
        sources = [held[0]] + [swap_mb(held[s], s) for s in range(1, count_mb)]
        arrived = [
            [swap_ma(piece, d) if d else piece for d, piece in enumerate(packed)]
            for packed in pack(here_ma, sources)
        ]
        every_state = relay_gather(states)
        here = scalars(here_ma, here_mb, here_ma, here_mb)
    else:
        mine = [lax.all_gather(first_branch_tensors, "ma", axis=2, tiled=True)]
        other = [lax.all_gather(second_branch_tensors, "ma", axis=2, tiled=True)]
        sent = jnp.transpose(pieces, (1, 0, 2, 3, 4, 5))
        sent = sent.reshape((groups,) + sent.shape[2:])
        arrived = lax.all_to_all(sent, AXES, split_axis=0, concat_axis=0, tiled=True)
        arrived = arrived.reshape((count_ma, count_mb) + arrived.shape[1:])
        arrived = [[arrived[d, :, :, l] for d in range(count_ma)] for l in range(local)]
        every_state = lax.all_gather(states, "ma", axis=0)
        every_state = [every_state[d] for d in range(count_ma)]
        here = scalars(0, here_mb, 0, 0)

    table, final_table, product = tables(
        here, relabel, mine, other, inner, count_mb, (short, True)
    )
    found = [[] for _ in range(0, count_ma, 2)]
    for l in range(local):
        own = contract_stem(arrived[l], table, product)
        stems = [own] + [swap_mb(own, s) for s in range(1, count_mb)]
        for pair, before in enumerate(found):
            chosen = every_state[2 * pair : 2 * pair + 2]
            found[pair] = contract_samples(chosen, stems, groups, l, local, before)
    found = [value for pair in found for value in pair]
    if short:
        found = [swap_ma(value, d) if d else value for d, value in enumerate(found)]
    else:
        found = lax.all_to_all(jnp.stack(found), "ma", split_axis=0, concat_axis=0, tiled=True)
        found = [found[d] for d in range(count_ma)]
    return contract_final(found, final_table).reshape(samples, parts, -1)


def solution(mesh):
    placed = (
        P(("cuts", "ma", "mb"), None, None, None),
        P(None, None, "ma", None),
        P(None, None, "ma", None),
        P(),
        P(("cuts", "ma", "mb"), None),
        P(("cuts", "ma", "mb"), None, None),
    )
    return jax.shard_map(
        on_device,
        mesh=mesh,
        in_specs=placed,
        out_specs=P(("cuts", "ma", "mb"), None, None),
        check_vma=False,
    )
```

```python
import functools

import jax
import jax.numpy as jnp
from jax import lax
from jax.experimental import pallas as pl
from jax.experimental.pallas import tpu as pltpu
from jax.sharding import PartitionSpec as P

AXES = ("ma", "mb")
BF16 = jnp.bfloat16
F32 = jnp.float32
VMEM = pl.BlockSpec(memory_space=pltpu.VMEM)
SMEM = pl.BlockSpec(memory_space=pltpu.SMEM)

LIMIT = 24 * 1024 * 1024


def params():
    return pltpu.CompilerParams(vmem_limit_bytes=LIMIT)


def permute(value, pairs):
    count = lax.axis_size("mb")
    full = [(a * count + c, b * count + c) for a, b in pairs for c in range(count)]
    return lax.ppermute(value, AXES, full)


def swap_ma(value, offset):
    return permute(value, [(m, m ^ offset) for m in range(lax.axis_size("ma"))])


def swap_mb(value, offset):
    count = lax.axis_size("ma") * lax.axis_size("mb")
    return lax.ppermute(value, AXES, [(m, m ^ offset) for m in range(count)])


def swap_cuts(value):
    shape = [lax.axis_size(name) for name in ("cuts",) + AXES]
    count, inner = shape[0], shape[1] * shape[2]
    pairs = [(c * inner + m, (c ^ 1) * inner + m) for c in range(count) for m in range(inner)]
    return lax.ppermute(value, ("cuts",) + AXES, pairs)


def relay_groups(length):
    owner, groups = {}, {}
    for distance in range(1, length):
        for z in range(length):
            for x in range(1, length):
                if abs((z ^ x) - z) != distance:
                    continue
                sender = z + (1 if (z ^ x) > z else -1)
                held = sender ^ z ^ x
                key = (x, owner.get((sender, held)))
                owner[(z, x)] = key
                groups.setdefault(key, []).append((sender, z))
    return groups


def relay_gather(value):
    length = lax.axis_size("ma") // 2
    sent = {None: value}
    slots = {0: [value]}
    for key, moves in relay_groups(length).items():
        pairs = [(2 * a + y, 2 * b + y) for a, b in moves for y in range(2)]
        sent[key] = permute(sent[key[1]], pairs)
        slots.setdefault(key[0], []).append(sent[key])
    gathered = {}
    for x in sorted(slots):
        whole = slots[x][0] if len(slots[x]) == 1 else merge(slots[x])
        gathered[2 * x] = whole
        gathered[2 * x + 1] = swap_ma(whole, 1)
    return [gathered[d] for d in range(2 * length)]


def merge_kernel(*refs):
    total = refs[0][...]
    for ref in refs[1:-1]:
        total = total + ref[...]
    refs[-1][...] = total


def merge(values):
    return pl.pallas_call(
        merge_kernel,
        in_specs=[VMEM] * len(values),
        out_specs=VMEM,
        out_shape=jax.ShapeDtypeStruct(values[0].shape, BF16),
        compiler_params=params(),
        name="merge",
    )(*values)


def scalars(*values):
    return jnp.stack([jnp.asarray(v, jnp.int32) for v in values])


def pack_kernel(offsets, blocks, place_ref, *refs):
    sources, outs = refs[: -len(offsets)], refs[-len(offsets) :]
    for d, out_ref in zip(offsets, outs):
        for s, source in enumerate(sources):
            seat = (place_ref[1],) if s == 0 else ()
            for number, l in enumerate(blocks):
                out_ref[number, s] = source[(l, place_ref[0] ^ d) + seat]


def pack(here, sources, offsets, blocks):
    shape = (len(blocks), len(sources)) + sources[0].shape[3:]
    return pl.pallas_call(
        functools.partial(pack_kernel, offsets, blocks),
        in_specs=[SMEM] + [VMEM] * len(sources),
        out_specs=[VMEM] * len(offsets),
        out_shape=[jax.ShapeDtypeStruct(shape, BF16)] * len(offsets),
        compiler_params=params(),
        name="pack",
    )(here, *sources)


def stack_kernel(*refs):
    for d, ref in enumerate(refs[:-1]):
        refs[-1][d] = ref[...]


def stack(values):
    return pl.pallas_call(
        stack_kernel,
        in_specs=[VMEM] * len(values),
        out_specs=VMEM,
        out_shape=jax.ShapeDtypeStruct((len(values),) + values[0].shape, BF16),
        compiler_params=params(),
        name="stack",
    )(*values)


def collect_kernel(place_ref, *refs):
    out_ref = refs[-1]
    stacks = len(refs) // 2
    count, _, depth, _ = refs[0].shape
    for number, ref in enumerate(refs[:-1]):
        turn = place_ref[1] if number < stacks else 1 - place_ref[1]
        for d in range(count):
            slot = (number % stacks) * count + d
            start = pl.multiple_of((place_ref[0] ^ slot) * depth, depth)
            out_ref[turn, :, pl.ds(start, depth), :] = ref[d]


def collect(here, own, far):
    count, parts, depth, width = own[0].shape
    return pl.pallas_call(
        collect_kernel,
        in_specs=[SMEM] + [VMEM] * (2 * len(own)),
        out_specs=VMEM,
        out_shape=jax.ShapeDtypeStruct((2, parts, depth * count * len(own), width), BF16),
        compiler_params=params(),
        name="collect",
    )(here, *own, *far)


def table_kernel(inner, count_mb, relative, slots, place_ref, relabel_ref, *refs):
    mine, other, refs = refs[:slots], refs[slots : 2 * slots], refs[2 * slots :]
    stem_ref, final_ref, product_ref, first_ref, second_ref, right_ref = refs
    depth = mine[0].shape[2]

    def gather(first, second):
        for d in range(slots):
            start = pl.multiple_of((place_ref[2] ^ d) * depth, depth)
            first_ref[:, :, pl.ds(start, depth), :] = first[d][...]
            second_ref[:, :, pl.ds(start, depth), :] = second[d][...]

    @pl.when(place_ref[3] == 0)
    def _():
        gather(mine, other)

    @pl.when(place_ref[3] != 0)
    def _():
        gather(other, mine)

    size = first_ref.shape[2]

    def select(near, relabel, repeat):
        column = lax.broadcasted_iota(jnp.int32, (repeat * size, size), 0) // repeat
        seat, rest = column // inner, column % inner
        ma, mb = seat // count_mb, seat % count_mb
        if near:
            ma, mb = ma ^ place_ref[0], mb ^ place_ref[1]
        position = (ma * count_mb + mb) * inner + rest
        return jnp.where(relabel == position, 1.0, 0.0).astype(BF16)

    selector = select(relative[0], relabel_ref[0:1, :], 2)
    real = jnp.dot(selector, first_ref[0, 0], preferred_element_type=F32)
    imag = jnp.dot(selector, first_ref[0, 1], preferred_element_type=F32)
    even = lax.broadcasted_iota(jnp.int32, real.shape, 0) % 2 == 0
    stem_ref[:size, :] = jnp.where(even, real, -imag).T.astype(BF16)
    stem_ref[size:, :] = jnp.where(even, imag, real).T.astype(BF16)
    selector = select(relative[1], relabel_ref[1:2, :], 1)
    real = jnp.dot(selector, first_ref[1, 0], preferred_element_type=F32).astype(BF16)
    imag = jnp.dot(selector, first_ref[1, 1], preferred_element_type=F32).astype(BF16)
    final_ref[:size, :size] = real
    final_ref[size:, size:] = real
    final_ref[:size, size:] = imag
    final_ref[size:, :size] = -imag
    width = second_ref.shape[2]
    right_ref[:width, :width] = second_ref[1, 0]
    right_ref[:width, width:] = second_ref[1, 1]
    right_ref[width:, :width] = -second_ref[1, 1]
    right_ref[width:, width:] = second_ref[1, 0]
    both = jnp.dot(second_ref[0, 0], right_ref[:width, :], preferred_element_type=F32)
    both += jnp.dot(second_ref[0, 1], right_ref[width:, :], preferred_element_type=F32)
    both = both.astype(BF16)
    product_ref[:width, :] = both
    product_ref[width:, :width] = -both[:, width:]
    product_ref[width:, width:] = both[:, :width]


def tables(here, relabel, mine, other, inner, count_mb, relative):
    rounds, parts, depth, width = mine[0].shape
    size = depth * len(mine)
    tensors = pltpu.VMEM((rounds, parts, size, width), BF16)
    return pl.pallas_call(
        functools.partial(table_kernel, inner, count_mb, relative, len(mine)),
        in_specs=[SMEM] + [VMEM] * (1 + 2 * len(mine)),
        out_specs=[VMEM] * 3,
        out_shape=[jax.ShapeDtypeStruct((2 * size, 2 * size), BF16)] * 3,
        scratch_shapes=[tensors, tensors, pltpu.VMEM((2 * size, 2 * size), BF16)],
        cost_estimate=pl.CostEstimate(
            flops=16 * size**3, bytes_accessed=40 * size * size, transcendentals=0
        ),
        compiler_params=params(),
        name="tables",
    )(here, relabel, *mine, *other)


def stem_kernel(blocks, *refs):
    arrived, (table_ref, product_ref, out_ref, rows_ref, mid_ref) = refs[:-5], refs[-5:]
    _, seats, depth, _ = arrived[0].shape
    for d, piece in enumerate(arrived):
        for s in range(seats):
            start = (d * seats + s) * depth
            rows_ref[start : start + depth, :] = piece[blocks[d], s]
    half = mid_ref.shape[0] // 2
    step = min(256, half)
    for top in range(0, 2 * half, step):
        part = jnp.dot(table_ref[top : top + step, :], rows_ref[...], preferred_element_type=F32)
        mid_ref[top : top + step, :] = part.astype(BF16)
    depth = mid_ref.shape[1]
    for top in range(0, half, step):
        part = jnp.dot(
            mid_ref[top : top + step, :], product_ref[:depth, :], preferred_element_type=F32
        )
        part += jnp.dot(
            mid_ref[half + top : half + top + step, :],
            product_ref[depth:, :],
            preferred_element_type=F32,
        )
        out_ref[top : top + step, :] = part.astype(BF16)


def contract_stem(arrived, table, product):
    arrived, blocks = zip(*arrived)
    width = arrived[0].shape[3]
    size = table.shape[0]
    return pl.pallas_call(
        functools.partial(stem_kernel, blocks),
        in_specs=[VMEM] * (len(arrived) + 2),
        out_specs=VMEM,
        out_shape=jax.ShapeDtypeStruct((size // 2, 2 * width), BF16),
        scratch_shapes=[pltpu.VMEM((size, width), BF16), pltpu.VMEM((size, width), BF16)],
        cost_estimate=pl.CostEstimate(
            flops=2 * (size * size * width + 2 * size * width * width),
            bytes_accessed=4 * (size * width + table.size),
            transcendentals=0,
        ),
        compiler_params=params(),
        name="contract_stem",
    )(*arrived, table, product)


def sample_kernel(groups, first, scale, many, seats, *refs):
    states, stems, refs = refs[:many], refs[many : many + seats], refs[many + seats :]
    before, outs = refs[: -2 - many], refs[-2 - many : -2]
    plus_ref, cross_ref = refs[-2:]
    depth = plus_ref.shape[0]
    width = depth // 2
    rows = stems[0].shape[0]
    inner = rows // groups
    step = min(256, rows)
    for m, state_ref in enumerate(states):
        plus_ref[:width, :] = state_ref[:width, :]
        plus_ref[width:, :] = -state_ref[width:depth, :]
        cross_ref[:width, :] = state_ref[width:depth, :]
        cross_ref[width:, :] = state_ref[:width, :]
        named = state_ref[depth : depth + 16, :].astype(F32)[:1, :]
        for s, stem_ref in enumerate(stems):
            for part, weights in enumerate((plus_ref, cross_ref)):
                total = before[m][s, part].astype(F32) if before else 0.0
                for top in range(0, rows, step):
                    value = jnp.dot(
                        stem_ref[top : top + step, :], weights[...], preferred_element_type=F32
                    )
                    for k in range(step // inner):
                        number = float((top // inner + k) * scale + first)
                        part_of = value[k * inner : (k + 1) * inner, :]
                        total += jnp.where(named == number, part_of, 0.0)
                outs[m][s, part] = total.astype(BF16)


def contract_samples(states, stems, groups, first, scale, before):
    many, seats = len(states), len(stems)
    _, samples = states[0].shape
    rows, width = stems[0].shape
    out = (seats, 2, rows // groups, samples)
    return pl.pallas_call(
        functools.partial(sample_kernel, groups, first, scale, many, seats),
        in_specs=[VMEM] * (many + seats + len(before)),
        out_specs=[VMEM] * many,
        out_shape=[jax.ShapeDtypeStruct(out, BF16)] * many,
        scratch_shapes=[pltpu.VMEM((width, samples), BF16)] * 2,
        cost_estimate=pl.CostEstimate(
            flops=2 * many * rows * width * 2 * samples * seats,
            bytes_accessed=2 * (many * states[0].size + seats * stems[0].size),
            transcendentals=0,
        ),
        compiler_params=params(),
        name="contract_samples",
    )(*states, *stems, *before)


def final_kernel(*refs):
    found, (table_ref, out_ref, rows_ref) = refs[:-3], refs[-3:]
    seats, parts, inner, _ = found[0].shape
    for d, piece in enumerate(found):
        for s in range(seats):
            for p in range(parts):
                start = ((p * len(found) + d) * seats + s) * inner
                rows_ref[start : start + inner, :] = piece[s, p]
    result = lax.dot_general(
        rows_ref[...], table_ref[...], (((0,), (0,)), ((), ())), preferred_element_type=F32
    ).astype(BF16)
    width = out_ref.shape[2]
    for p in range(parts):
        out_ref[:, p, :] = result[:, p * width : (p + 1) * width]


def contract_final(found, table):
    parts, _, samples = found[0].shape[1:]
    return pl.pallas_call(
        final_kernel,
        in_specs=[VMEM] * (len(found) + 1),
        out_specs=VMEM,
        out_shape=jax.ShapeDtypeStruct((samples, parts, table.shape[1] // parts), BF16),
        scratch_shapes=[pltpu.VMEM((table.shape[0], samples), BF16)],
        cost_estimate=pl.CostEstimate(
            flops=2 * table.size * samples, bytes_accessed=2 * table.size, transcendentals=0
        ),
        compiler_params=params(),
        name="contract_final",
    )(*found, table)


def is_short(count_cuts, count_ma, rounds):
    return count_ma // 2 <= 4 and count_cuts == rounds == 2


def on_device(
    stem_field, first_branch_tensors, second_branch_tensors, relabel, sample_block, sample_state
):
    count_ma, count_mb = lax.axis_size("ma"), lax.axis_size("mb")
    here_ma, here_mb = lax.axis_index("ma"), lax.axis_index("mb")
    groups = count_ma * count_mb
    local, row_count, parts, width = stem_field.shape
    inner = row_count // groups
    samples = sample_state.shape[0]
    short = is_short(lax.axis_size("cuts"), count_ma, first_branch_tensors.shape[0])
    here_cuts = lax.axis_index("cuts")

    flat = sample_state.reshape(samples, parts * width).T
    named = jnp.broadcast_to(sample_block[:, 0].astype(BF16)[None, :], (16, samples))
    states = jnp.concatenate([flat, named], axis=0)

    pieces = stem_field.reshape(local, count_ma, count_mb, inner * parts, width)

    if short:
        share = jnp.where(here_mb == 0, first_branch_tensors, second_branch_tensors)
        share = lax.dynamic_index_in_dim(share, here_cuts, keepdims=False)
        own = [swap_ma(share, d) if d else share for d in range(count_ma)]
        half = count_ma // 2
        own = [stack(own[:half]), stack(own[half:])]
        far = [swap_cuts(value) for value in own]
        mine = collect(scalars(here_ma, here_cuts), own, far)
        other = swap_mb(mine, 1)
        mine, other = [mine], [other]
        sources = [pieces]
        for s in range(1, count_mb):
            held = lax.dynamic_index_in_dim(pieces, here_mb ^ s, 2, keepdims=False)
            sources.append(swap_mb(held, s))
        place = scalars(here_ma, here_mb)
        near, distant = tuple(range(half)), tuple(range(half, count_ma))
        arrived = [[] for _ in range(local)]
        for d, piece in zip(near, pack(place, sources, near, tuple(range(local)))):
            piece = swap_ma(piece, d) if d else piece
            for l in range(local):
                arrived[l].append((piece, l))
        for l in range(local):
            for d, piece in zip(distant, pack(place, sources, distant, (l,))):
                arrived[l].append((swap_ma(piece, d), 0))
        every_state = relay_gather(states)
        here = scalars(here_ma, here_mb, 0, here_mb)
    else:
        mine = [lax.all_gather(first_branch_tensors, "ma", axis=2, tiled=True)]
        other = [lax.all_gather(second_branch_tensors, "ma", axis=2, tiled=True)]
        sent = jnp.transpose(pieces, (1, 2, 0, 3, 4))
        sent = sent.reshape((groups,) + sent.shape[2:])
        arrived = lax.all_to_all(sent, AXES, split_axis=0, concat_axis=0, tiled=True)
        arrived = arrived.reshape((count_ma, count_mb) + arrived.shape[1:])
        arrived = [[(arrived[d, :, l][None], 0) for d in range(count_ma)] for l in range(local)]
        every_state = lax.all_gather(states, "ma", axis=0)
        every_state = [every_state[d] for d in range(count_ma)]
        here = scalars(0, here_mb, 0, 0)

    table, final_table, product = tables(
        here, relabel, mine, other, inner, count_mb, (short, True)
    )
    found = [[] for _ in range(0, count_ma, 2)]
    for l in range(local):
        own = contract_stem(arrived[l], table, product)
        stems = [own] + [swap_mb(own, s) for s in range(1, count_mb)]
        for pair, before in enumerate(found):
            chosen = every_state[2 * pair : 2 * pair + 2]
            found[pair] = contract_samples(chosen, stems, groups, l, local, before)
    found = [value for pair in found for value in pair]
    if short:
        found = [swap_ma(value, d) if d else value for d, value in enumerate(found)]
    else:
        found = lax.all_to_all(jnp.stack(found), "ma", split_axis=0, concat_axis=0, tiled=True)
        found = [found[d] for d in range(count_ma)]
    return contract_final(found, final_table)


def solution(mesh):
    placed = (
        P(("cuts", "ma", "mb"), None, None, None),
        P(None, None, "ma", None),
        P(None, None, "ma", None),
        P(),
        P(("cuts", "ma", "mb"), None),
        P(("cuts", "ma", "mb"), None, None),
    )
    step = jax.shard_map(
        on_device,
        mesh=mesh,
        in_specs=placed,
        out_specs=P(("cuts", "ma", "mb"), None, None),
        check_vma=False,
    )
    if not is_short(mesh.shape["cuts"], mesh.shape["ma"], 2):
        return step
    return step
```

```python
import functools

import jax
import jax.numpy as jnp
from jax import lax
from jax.experimental import pallas as pl
from jax.experimental.pallas import tpu as pltpu
from jax.sharding import PartitionSpec as P

AXES = ("ma", "mb")
BF16 = jnp.bfloat16
F32 = jnp.float32
VMEM = pl.BlockSpec(memory_space=pltpu.VMEM)
SMEM = pl.BlockSpec(memory_space=pltpu.SMEM)

LIMIT = 24 * 1024 * 1024


def params():
    return pltpu.CompilerParams(vmem_limit_bytes=LIMIT)


def permute(value, pairs):
    count = lax.axis_size("mb")
    full = [(a * count + c, b * count + c) for a, b in pairs for c in range(count)]
    return lax.ppermute(value, AXES, full)


def swap_ma(value, offset):
    return permute(value, [(m, m ^ offset) for m in range(lax.axis_size("ma"))])


def swap_mb(value, offset):
    count = lax.axis_size("ma") * lax.axis_size("mb")
    return lax.ppermute(value, AXES, [(m, m ^ offset) for m in range(count)])


def swap_cuts(value):
    shape = [lax.axis_size(name) for name in ("cuts",) + AXES]
    count, inner = shape[0], shape[1] * shape[2]
    pairs = [(c * inner + m, (c ^ 1) * inner + m) for c in range(count) for m in range(inner)]
    return lax.ppermute(value, ("cuts",) + AXES, pairs)


def relay_groups(length):
    owner, groups = {}, {}
    for distance in range(1, length):
        for z in range(length):
            for x in range(1, length):
                if abs((z ^ x) - z) != distance:
                    continue
                sender = z + (1 if (z ^ x) > z else -1)
                held = sender ^ z ^ x
                key = (x, owner.get((sender, held)))
                owner[(z, x)] = key
                groups.setdefault(key, []).append((sender, z))
    return groups


def relay_gather(value):
    length = lax.axis_size("ma") // 2
    sent = {None: value}
    slots = {0: [value]}
    for key, moves in relay_groups(length).items():
        pairs = [(2 * a + y, 2 * b + y) for a, b in moves for y in range(2)]
        sent[key] = permute(sent[key[1]], pairs)
        slots.setdefault(key[0], []).append(sent[key])
    gathered = {}
    for x in sorted(slots):
        whole = slots[x][0] if len(slots[x]) == 1 else merge(slots[x])
        gathered[2 * x] = whole
        gathered[2 * x + 1] = swap_ma(whole, 1)
    return [gathered[d] for d in range(2 * length)]


def merge_kernel(*refs):
    total = refs[0][...]
    for ref in refs[1:-1]:
        total = total + ref[...]
    refs[-1][...] = total


def merge(values):
    return pl.pallas_call(
        merge_kernel,
        in_specs=[VMEM] * len(values),
        out_specs=VMEM,
        out_shape=jax.ShapeDtypeStruct(values[0].shape, BF16),
        compiler_params=params(),
        name="merge",
    )(*values)


def scalars(*values):
    return jnp.stack([jnp.asarray(v, jnp.int32) for v in values])


def pack_kernel(offsets, blocks, place_ref, *refs):
    sources, outs = refs[: -len(offsets)], refs[-len(offsets) :]
    for d, out_ref in zip(offsets, outs):
        for s, source in enumerate(sources):
            seat = (place_ref[1],) if s == 0 else ()
            for number, l in enumerate(blocks):
                out_ref[number, s] = source[(l, place_ref[0] ^ d) + seat]


def pack(here, sources, offsets, blocks):
    shape = (len(blocks), len(sources)) + sources[0].shape[3:]
    return pl.pallas_call(
        functools.partial(pack_kernel, offsets, blocks),
        in_specs=[SMEM] + [VMEM] * len(sources),
        out_specs=[VMEM] * len(offsets),
        out_shape=[jax.ShapeDtypeStruct(shape, BF16)] * len(offsets),
        compiler_params=params(),
        name="pack",
    )(here, *sources)


def stack_kernel(*refs):
    for d, ref in enumerate(refs[:-1]):
        refs[-1][d] = ref[...]


def stack(values):
    return pl.pallas_call(
        stack_kernel,
        in_specs=[VMEM] * len(values),
        out_specs=VMEM,
        out_shape=jax.ShapeDtypeStruct((len(values),) + values[0].shape, BF16),
        compiler_params=params(),
        name="stack",
    )(*values)


def collect_kernel(place_ref, *refs):
    out_ref = refs[-1]
    stacks = len(refs) // 2
    count, _, depth, _ = refs[0].shape
    for number, ref in enumerate(refs[:-1]):
        turn = place_ref[1] if number < stacks else 1 - place_ref[1]
        for d in range(count):
            slot = (number % stacks) * count + d
            start = pl.multiple_of((place_ref[0] ^ slot) * depth, depth)
            out_ref[turn, :, pl.ds(start, depth), :] = ref[d]


def collect(here, own, far):
    count, parts, depth, width = own[0].shape
    return pl.pallas_call(
        collect_kernel,
        in_specs=[SMEM] + [VMEM] * (2 * len(own)),
        out_specs=VMEM,
        out_shape=jax.ShapeDtypeStruct((2, parts, depth * count * len(own), width), BF16),
        compiler_params=params(),
        name="collect",
    )(here, *own, *far)


def table_kernel(inner, count_mb, relative, slots, place_ref, relabel_ref, *refs):
    mine, other, refs = refs[:slots], refs[slots : 2 * slots], refs[2 * slots :]
    stem_ref, final_ref, product_ref, first_ref, second_ref, right_ref = refs
    depth = mine[0].shape[2]

    def gather(first, second):
        for d in range(slots):
            start = pl.multiple_of((place_ref[2] ^ d) * depth, depth)
            first_ref[:, :, pl.ds(start, depth), :] = first[d][...]
            second_ref[:, :, pl.ds(start, depth), :] = second[d][...]

    @pl.when(place_ref[3] == 0)
    def _():
        gather(mine, other)

    @pl.when(place_ref[3] != 0)
    def _():
        gather(other, mine)

    size = first_ref.shape[2]

    def select(near, relabel, repeat):
        column = lax.broadcasted_iota(jnp.int32, (repeat * size, size), 0) // repeat
        seat, rest = column // inner, column % inner
        ma, mb = seat // count_mb, seat % count_mb
        if near:
            ma, mb = ma ^ place_ref[0], mb ^ place_ref[1]
        position = (ma * count_mb + mb) * inner + rest
        return jnp.where(relabel == position, 1.0, 0.0).astype(BF16)

    selector = select(relative[0], relabel_ref[0:1, :], 2)
    real = jnp.dot(selector, first_ref[0, 0], preferred_element_type=F32)
    imag = jnp.dot(selector, first_ref[0, 1], preferred_element_type=F32)
    even = lax.broadcasted_iota(jnp.int32, real.shape, 0) % 2 == 0
    stem_ref[:size, :] = jnp.where(even, real, -imag).T.astype(BF16)
    stem_ref[size:, :] = jnp.where(even, imag, real).T.astype(BF16)
    selector = select(relative[1], relabel_ref[1:2, :], 1)
    real = jnp.dot(selector, first_ref[1, 0], preferred_element_type=F32).astype(BF16)
    imag = jnp.dot(selector, first_ref[1, 1], preferred_element_type=F32).astype(BF16)
    final_ref[:size, :size] = real
    final_ref[size:, size:] = real
    final_ref[:size, size:] = imag
    final_ref[size:, :size] = -imag
    width = second_ref.shape[2]
    right_ref[:width, :width] = second_ref[1, 0]
    right_ref[:width, width:] = second_ref[1, 1]
    right_ref[width:, :width] = -second_ref[1, 1]
    right_ref[width:, width:] = second_ref[1, 0]
    both = jnp.dot(second_ref[0, 0], right_ref[:width, :], preferred_element_type=F32)
    both += jnp.dot(second_ref[0, 1], right_ref[width:, :], preferred_element_type=F32)
    both = both.astype(BF16)
    product_ref[:width, :] = both
    product_ref[width:, :width] = -both[:, width:]
    product_ref[width:, width:] = both[:, :width]


def tables(here, relabel, mine, other, inner, count_mb, relative):
    rounds, parts, depth, width = mine[0].shape
    size = depth * len(mine)
    tensors = pltpu.VMEM((rounds, parts, size, width), BF16)
    return pl.pallas_call(
        functools.partial(table_kernel, inner, count_mb, relative, len(mine)),
        in_specs=[SMEM] + [VMEM] * (1 + 2 * len(mine)),
        out_specs=[VMEM] * 3,
        out_shape=[jax.ShapeDtypeStruct((2 * size, 2 * size), BF16)] * 3,
        scratch_shapes=[tensors, tensors, pltpu.VMEM((2 * size, 2 * size), BF16)],
        cost_estimate=pl.CostEstimate(
            flops=16 * size**3, bytes_accessed=40 * size * size, transcendentals=0
        ),
        compiler_params=params(),
        name="tables",
    )(here, relabel, *mine, *other)


def stem_kernel(blocks, *refs):
    arrived, (table_ref, product_ref, out_ref, rows_ref, mid_ref) = refs[:-5], refs[-5:]
    _, seats, depth, _ = arrived[0].shape
    for d, piece in enumerate(arrived):
        for s in range(seats):
            start = (d * seats + s) * depth
            rows_ref[start : start + depth, :] = piece[blocks[d], s]
    half = mid_ref.shape[0] // 2
    step = min(256, half)
    for top in range(0, 2 * half, step):
        part = jnp.dot(table_ref[top : top + step, :], rows_ref[...], preferred_element_type=F32)
        mid_ref[top : top + step, :] = part.astype(BF16)
    depth = mid_ref.shape[1]
    for top in range(0, half, step):
        part = jnp.dot(
            mid_ref[top : top + step, :], product_ref[:depth, :], preferred_element_type=F32
        )
        part += jnp.dot(
            mid_ref[half + top : half + top + step, :],
            product_ref[depth:, :],
            preferred_element_type=F32,
        )
        out_ref[top : top + step, :] = part.astype(BF16)


def contract_stem(arrived, table, product):
    arrived, blocks = zip(*arrived)
    width = arrived[0].shape[3]
    size = table.shape[0]
    return pl.pallas_call(
        functools.partial(stem_kernel, blocks),
        in_specs=[VMEM] * (len(arrived) + 2),
        out_specs=VMEM,
        out_shape=jax.ShapeDtypeStruct((size // 2, 2 * width), BF16),
        scratch_shapes=[pltpu.VMEM((size, width), BF16), pltpu.VMEM((size, width), BF16)],
        cost_estimate=pl.CostEstimate(
            flops=2 * (size * size * width + 2 * size * width * width),
            bytes_accessed=4 * (size * width + table.size),
            transcendentals=0,
        ),
        compiler_params=params(),
        name="contract_stem",
    )(*arrived, table, product)


def sample_kernel(groups, first, scale, many, seats, *refs):
    states, stems, refs = refs[:many], refs[many : many + seats], refs[many + seats :]
    before, outs = refs[: -2 - many], refs[-2 - many : -2]
    plus_ref, cross_ref = refs[-2:]
    depth = plus_ref.shape[0]
    width = depth // 2
    rows = stems[0].shape[0]
    inner = rows // groups
    step = min(256, rows)
    for m, state_ref in enumerate(states):
        plus_ref[:width, :] = state_ref[:width, :]
        plus_ref[width:, :] = -state_ref[width:depth, :]
        cross_ref[:width, :] = state_ref[width:depth, :]
        cross_ref[width:, :] = state_ref[:width, :]
        named = state_ref[depth : depth + 16, :].astype(F32)[:1, :]
        for s, stem_ref in enumerate(stems):
            for part, weights in enumerate((plus_ref, cross_ref)):
                total = before[m][s, part].astype(F32) if before else 0.0
                for top in range(0, rows, step):
                    value = jnp.dot(
                        stem_ref[top : top + step, :], weights[...], preferred_element_type=F32
                    )
                    for k in range(step // inner):
                        number = float((top // inner + k) * scale + first)
                        part_of = value[k * inner : (k + 1) * inner, :]
                        total += jnp.where(named == number, part_of, 0.0)
                outs[m][s, part] = total.astype(BF16)


def contract_samples(states, stems, groups, first, scale, before):
    many, seats = len(states), len(stems)
    _, samples = states[0].shape
    rows, width = stems[0].shape
    out = (seats, 2, rows // groups, samples)
    return pl.pallas_call(
        functools.partial(sample_kernel, groups, first, scale, many, seats),
        in_specs=[VMEM] * (many + seats + len(before)),
        out_specs=[VMEM] * many,
        out_shape=[jax.ShapeDtypeStruct(out, BF16)] * many,
        scratch_shapes=[pltpu.VMEM((width, samples), BF16)] * 2,
        cost_estimate=pl.CostEstimate(
            flops=2 * many * rows * width * 2 * samples * seats,
            bytes_accessed=2 * (many * states[0].size + seats * stems[0].size),
            transcendentals=0,
        ),
        compiler_params=params(),
        name="contract_samples",
    )(*states, *stems, *before)


def final_kernel(first, count, *refs):
    found, table_ref = refs[:count], refs[count]
    before, (out_ref, rows_ref) = refs[count + 1 : -2], refs[-2:]
    seats, parts, inner, _ = found[0].shape
    block = len(found) * seats * inner
    for d, piece in enumerate(found):
        for s in range(seats):
            for p in range(parts):
                start = p * block + (d * seats + s) * inner
                rows_ref[start : start + inner, :] = piece[s, p]
    total = before[0][...] if before else 0.0
    half = table_ref.shape[0] // parts
    offset = first * seats * inner
    for p in range(parts):
        total += lax.dot_general(
            rows_ref[p * block : (p + 1) * block, :],
            table_ref[p * half + offset : p * half + offset + block, :],
            (((0,), (0,)), ((), ())),
            preferred_element_type=F32,
        )
    if out_ref.ndim == 2:
        out_ref[...] = total
    else:
        result = total.astype(BF16)
        width = out_ref.shape[2]
        for p in range(parts):
            out_ref[:, p, :] = result[:, p * width : (p + 1) * width]


def contract_final(found, table, first, before):
    seats, parts, inner, samples = found[0].shape
    last = (first + len(found)) * seats * inner * parts == table.shape[0]
    shape = (samples, parts, table.shape[1] // parts) if last else (samples, table.shape[1])
    rows = len(found) * seats * parts * inner
    return pl.pallas_call(
        functools.partial(final_kernel, first, len(found)),
        in_specs=[VMEM] * (len(found) + 1 + len(before)),
        out_specs=VMEM,
        out_shape=jax.ShapeDtypeStruct(shape, BF16 if last else F32),
        scratch_shapes=[pltpu.VMEM((rows, samples), BF16)],
        cost_estimate=pl.CostEstimate(
            flops=2 * rows * samples * table.shape[1],
            bytes_accessed=2 * rows * table.shape[1],
            transcendentals=0,
        ),
        compiler_params=params(),
        name="contract_final",
    )(*found, table, *before)


def is_short(count_cuts, count_ma, rounds):
    return count_ma // 2 <= 4 and count_cuts == rounds == 2


def on_device(
    stem_field, first_branch_tensors, second_branch_tensors, relabel, sample_block, sample_state
):
    count_ma, count_mb = lax.axis_size("ma"), lax.axis_size("mb")
    here_ma, here_mb = lax.axis_index("ma"), lax.axis_index("mb")
    groups = count_ma * count_mb
    local, row_count, parts, width = stem_field.shape
    inner = row_count // groups
    samples = sample_state.shape[0]
    short = is_short(lax.axis_size("cuts"), count_ma, first_branch_tensors.shape[0])
    here_cuts = lax.axis_index("cuts")

    flat = sample_state.reshape(samples, parts * width).T
    named = jnp.broadcast_to(sample_block[:, 0].astype(BF16)[None, :], (16, samples))
    states = jnp.concatenate([flat, named], axis=0)

    pieces = stem_field.reshape(local, count_ma, count_mb, inner * parts, width)

    if short:
        share = jnp.where(here_mb == 0, first_branch_tensors, second_branch_tensors)
        share = lax.dynamic_index_in_dim(share, here_cuts, keepdims=False)
        own = [swap_ma(share, d) if d else share for d in range(count_ma)]
        half = count_ma // 2
        own = [stack(own[:half]), stack(own[half:])]
        far = [swap_cuts(value) for value in own]
        mine = collect(scalars(here_ma, here_cuts), own, far)
        other = swap_mb(mine, 1)
        mine, other = [mine], [other]
        sources = [pieces]
        for s in range(1, count_mb):
            held = lax.dynamic_index_in_dim(pieces, here_mb ^ s, 2, keepdims=False)
            sources.append(swap_mb(held, s))
        place = scalars(here_ma, here_mb)
        near, distant = tuple(range(half)), tuple(range(half, count_ma))
        arrived = [[] for _ in range(local)]
        for d, piece in zip(near, pack(place, sources, near, tuple(range(local)))):
            piece = swap_ma(piece, d) if d else piece
            for l in range(local):
                arrived[l].append((piece, l))
        for l in range(local):
            for d, piece in zip(distant, pack(place, sources, distant, (l,))):
                arrived[l].append((swap_ma(piece, d), 0))
        every_state = relay_gather(states)
        here = scalars(here_ma, here_mb, 0, here_mb)
    else:
        mine = [lax.all_gather(first_branch_tensors, "ma", axis=2, tiled=True)]
        other = [lax.all_gather(second_branch_tensors, "ma", axis=2, tiled=True)]
        sent = jnp.transpose(pieces, (1, 2, 0, 3, 4))
        sent = sent.reshape((groups,) + sent.shape[2:])
        arrived = lax.all_to_all(sent, AXES, split_axis=0, concat_axis=0, tiled=True)
        arrived = arrived.reshape((count_ma, count_mb) + arrived.shape[1:])
        arrived = [[(arrived[d, :, l][None], 0) for d in range(count_ma)] for l in range(local)]
        every_state = lax.all_gather(states, "ma", axis=0)
        every_state = [every_state[d] for d in range(count_ma)]
        here = scalars(0, here_mb, 0, 0)

    table, final_table, product = tables(
        here, relabel, mine, other, inner, count_mb, (short, True)
    )
    found = [[] for _ in range(0, count_ma, 2)]
    for l in range(local):
        own = contract_stem(arrived[l], table, product)
        stems = [own] + [swap_mb(own, s) for s in range(1, count_mb)]
        for pair, before in enumerate(found):
            chosen = every_state[2 * pair : 2 * pair + 2]
            found[pair] = contract_samples(chosen, stems, groups, l, local, before)
    found = [value for pair in found for value in pair]
    if short:
        found = [swap_ma(value, d) if d else value for d, value in enumerate(found)]
    else:
        found = lax.all_to_all(jnp.stack(found), "ma", split_axis=0, concat_axis=0, tiled=True)
        found = [found[d] for d in range(count_ma)]
    cut = count_ma - 2
    sums = contract_final(found[:cut], final_table, 0, [])
    return contract_final(found[cut:], final_table, cut, [sums])


def solution(mesh):
    placed = (
        P(("cuts", "ma", "mb"), None, None, None),
        P(None, None, "ma", None),
        P(None, None, "ma", None),
        P(),
        P(("cuts", "ma", "mb"), None),
        P(("cuts", "ma", "mb"), None, None),
    )
    step = jax.shard_map(
        on_device,
        mesh=mesh,
        in_specs=placed,
        out_specs=P(("cuts", "ma", "mb"), None, None),
        check_vma=False,
    )
    if not is_short(mesh.shape["cuts"], mesh.shape["ma"], 2):
        return step
    return step
```
